32 devices in a mesh: sector: 8 (over z, core), cap: 4 (over y, x).
Axes of the slice: x: 2, y: 2, z: 4, core: 2. Of those that a mesh axis runs over, the one named last changes fastest.
Arguments:
- start_value: float32 [64, 32, 2048], P('sector', None, 'cap'), may hold values from 0 to 4
- firm_mass: float32 [64, 32, 2048], P('sector', None, 'cap'), may hold values from 0.1 to 10
- survive: int32 [64, 32, 2048], P('sector', None, 'cap'), may hold values from 0 to 1, as said below
- exit_index: int32 [64], P('sector'), may hold values from 0 to 8
- demand: float32 [64], P('sector'), may hold values from 0.3 to 90, as said below
- transition: float32 [32, 32], replicated, may hold values from 0 to 1, as said below
- install_cost: float32 [2048], P('cap'), may hold values from 0 to 1
Outputs:
- final_value: float32 [64, 32, 2048], P('sector', None, 'cap')
- rel_prices: float32 [64], P('sector')
The draws below stay inside these ranges and needn't reach their ends.
Inputs may be any that keep to these rules, and one draw needn't show every extreme that they name: `survive`: 0 or 1; the share of ones differs from sector to sector, from about a tenth to all. `demand`: positive, rising over the sectors by some thirty times. `transition`: entries positive, every row sums to one.
All inputs are finite; a program needn't handle non-finite values.
Results may differ from the reference program's by a relative error of at most 0.0003.
Values sent between devices are 32-bit elements; how exact they have to be, the bound alone decides.
A program may use at most 64 MiB of HBM per device.

```python
import math
import jax
import jax.numpy as jnp
from jax import lax

K = 2048
Z = 32
SWEEPS = 2
S = 64


def draw_survive(key, part):
    first_key, second_key = jax.random.split(jax.random.fold_in(key, 11))
    shares = jax.random.randint(first_key, (S, 1, 1), 10, 101)
    rolled = jax.random.randint(second_key, (S, Z, K), 0, 100)
    return (rolled < shares).astype(jnp.int32)


def draw_demand(key, part):
    sector_pos = jnp.arange(S).astype(jnp.float32)
    base = jnp.exp(jnp.log(30.0) * sector_pos / max(S - 1, 1))
    noise = jax.random.uniform(jax.random.fold_in(key, 21), (S,), minval=-0.5, maxval=0.5)
    return (base * jnp.exp(noise)).astype(jnp.float32)


def draw_transition(key, part):
    states = jnp.arange(Z)
    spread = jnp.abs(states[:, None] - states[None, :]).astype(jnp.float32)
    raw = jax.random.uniform(jax.random.fold_in(key, 31), (Z, Z), minval=0.3, maxval=1.0) * jnp.exp(-spread / 4.0)
    raw = raw + jnp.eye(Z, dtype=jnp.float32)
    return (raw / jnp.sum(raw, axis=1, keepdims=True)).astype(jnp.float32)


def touch_ends(values, own_key, smallest, top_value):
    shape = values.shape
    spot = [jax.random.randint(jax.random.fold_in(own_key, axis), (), 0, shape[axis]) for axis in range(len(shape))]
    values = values.at[tuple(spot)].set(smallest)
    longest = shape.index(max(shape))
    spot[longest] = (spot[longest] + 1) % shape[longest]
    return values.at[tuple(spot)].set(top_value)


def levels(own_key, dims, cuts, least, high):
    loudness, own = 1.0, jax.random.fold_in(own_key, 6)
    for position, blocks in cuts:
        steps = jnp.exp(jax.random.uniform(jax.random.fold_in(own, position), (blocks,), jnp.float32, least / len(cuts), high / len(cuts)))
        loudness = loudness * jnp.repeat(steps, dims[position] // blocks).reshape([-1 if axis == position else 1 for axis in range(len(dims))])
    return loudness


def setup_inputs(seed: int = 0) -> dict:
    arg_keys = jax.random.split(jax.random.key(seed), 8)
    start_value = jnp.clip(4.0 * jax.random.uniform(arg_keys[0], (S, Z, K), jnp.float32) ** levels(arg_keys[0], (S, Z, K), ((0, 8), (2, 4)), -0.2, 0.2), 0.0, 4.0)
    firm_mass = jnp.clip(jnp.exp(math.log(10.0) - 4.6051702 * jax.random.uniform(arg_keys[1], (S, Z, K), jnp.float32) ** levels(arg_keys[1], (S, Z, K), ((0, 8), (2, 4)), -0.2, 0.2)), 0.1, 10.0)
    survive = draw_survive(jax.random.fold_in(arg_keys[7], 71), 0)
    exit_index = touch_ends(jax.random.randint(arg_keys[3], (S,), 0, Z // 4 + 1), jax.random.fold_in(arg_keys[3], 1), 0, (Z // 4 + 1) - 1).astype(jnp.int32)
    demand = draw_demand(jax.random.fold_in(arg_keys[7], 71), 0)
    transition = draw_transition(jax.random.fold_in(arg_keys[7], 71), 0)
    install_cost = jnp.clip(1.0 * jax.random.uniform(arg_keys[6], (K,), jnp.float32) ** levels(arg_keys[6], (K,), ((0, 4),), -0.2, 0.2), 0.0, 1.0)
    return dict(start_value=start_value, firm_mass=firm_mass, survive=survive, exit_index=exit_index, demand=demand, transition=transition, install_cost=install_cost)


def capital_of(positions):
    return 0.2 * jnp.exp(jnp.log(10.0) * positions.astype(jnp.float32) / (K - 1))

def charge_of(cap_now, cap_next, row_ids, col_ids):
    invest = cap_next - 0.9 * cap_now
    fixed = jnp.where(row_ids == col_ids, 0.0, 1.5 * cap_now)
    return invest + invest * invest / cap_now + fixed

def sector_best(forward_value):
    row_block = math.gcd(K, 256)
    col_ids = jnp.arange(K, dtype=jnp.int32)
    capital = capital_of(col_ids)

    def row_step(first_row):
        row_ids = first_row + jnp.arange(row_block, dtype=jnp.int32)
        rows = capital_of(row_ids)
        charge = charge_of(rows[:, None], capital[None, :], row_ids[:, None], col_ids[None, :])
        return lax.optimization_barrier(jnp.max(forward_value[:, None, :] - charge[None], axis=2))
    starts = (jnp.arange(K // row_block) * row_block).astype(jnp.int32)
    blocks = lax.map(row_step, starts)
    return blocks.transpose(1, 0, 2).reshape(Z, K)

def reference(start_value, firm_mass, survive, exit_index, demand, transition, install_cost):
    prod_index = jnp.arange(Z, dtype=jnp.int32)
    capital = capital_of(jnp.arange(K, dtype=jnp.int32))
    log_prod = -0.5 + prod_index.astype(jnp.float32) / (Z - 1)
    output = jnp.exp(log_prod)[:, None] * capital[None, :] ** 0.6
    scrap = 0.3 * capital
    live = (survive == 1) & (prod_index[None, :, None] >= exit_index[:, None, None])
    values = start_value
    relative = jnp.zeros((S,), jnp.float32)
    for sweep in range(SWEEPS):
        staying = jnp.where(live, jax.nn.sigmoid((values - scrap) / 0.5), 0.0)
        supply = 1.0 + lax.optimization_barrier(jnp.sum(firm_mass * staying * output, axis=(1, 2))) / (Z * K)
        prices = jnp.sqrt(demand / supply)
        price_index = jnp.mean(jnp.sqrt(prices)) ** 2
        relative = prices / price_index
        continuation = jnp.where(live, jnp.maximum(values, scrap), scrap)
        expect = jnp.einsum('zw,swk->szk', transition, continuation, precision=lax.Precision.HIGHEST)
        forward_value = 0.9 * expect - install_cost[None, None, :]
        best = lax.map(sector_best, forward_value)
        values = jnp.where(live, relative[:, None, None] * output + best, scrap)
    return (values, relative)
```

```python
import functools
import math

import jax
import jax.numpy as jnp
from jax import lax
from jax.experimental import pallas as pl
from jax.experimental.pallas import tpu as pltpu
from jax.sharding import PartitionSpec as P

SWEEPS = 2
SLOTS = 16
NEG = -1e30


def capital_of(positions, total):
    return 0.2 * jnp.exp(math.log(10.0) * positions.astype(jnp.float32) / (total - 1))


def charge_of(cap_now, cap_next, row_ids, col_ids):
    invest = cap_next - 0.9 * cap_now
    fixed = jnp.where(row_ids == col_ids, 0.0, 1.5 * cap_now)
    return invest + invest * invest / cap_now + fixed


def best_reply(forward_rows, row_first, row_count):
    total_rows, total_cols = forward_rows.shape
    cap_of = functools.partial(capital_of, total=total_cols)
    col_block = math.gcd(total_cols, 2048)
    row_block = math.gcd(row_count, 512)
    grp_limit = max(1, (1 << 24) // (row_block * col_block))
    grp_size = math.gcd(total_rows, 1 << min(total_rows, grp_limit).bit_length() - 1)
    groups = forward_rows.reshape(total_rows // grp_size, grp_size, total_cols)

    def one_group(group):
        row_ids = row_first + 0 * row_block + jnp.arange(row_block, dtype=jnp.int32)
        cap_rows = cap_of(row_ids)
        empty = jnp.full((grp_size, row_block), -1e30, jnp.float32)
        col_ids = jnp.arange(col_block, dtype=jnp.int32)
        cap_cols = cap_of(col_ids)
        charge = charge_of(cap_rows[:, None], cap_cols[None, :], row_ids[:, None], col_ids[None, :])
        return jnp.maximum(empty, jnp.max(group[:, None, :] - charge[None], axis=2))

    return lax.map(one_group, groups).reshape(total_rows, row_count)


def dense_sweeps(start_value, firm_mass, survive, exit_index, demand, transition, install_cost):
    sec_dev, prod_count, cap_dev = start_value.shape
    sectors_all = sec_dev * lax.axis_size("sector")
    row_first = lax.axis_index("cap") * cap_dev
    prod_index = jnp.arange(prod_count, dtype=jnp.int32)
    total = cap_dev * lax.axis_size("cap")
    capital = capital_of(row_first + jnp.arange(cap_dev, dtype=jnp.int32), total)
    log_prod = -0.5 + prod_index.astype(jnp.float32) / (prod_count - 1)
    output = jnp.exp(log_prod)[:, None] * capital[None, :] ** 0.6
    scrap = 0.3 * capital
    live = (survive == 1) & (prod_index[None, :, None] >= exit_index[:, None, None])
    values = start_value
    relative = jnp.zeros((sec_dev,), jnp.float32)
    for sweep in range(SWEEPS):
        staying = jnp.where(live, jax.nn.sigmoid((values - scrap) / 0.5), 0.0)
        partial_value = jnp.sum(firm_mass * staying * output, axis=(1, 2))
        supply = 1.0 + lax.psum(partial_value, "cap") / (prod_count * total)
        prices = jnp.sqrt(demand / supply)
        root_sum = lax.psum(jnp.sum(jnp.sqrt(prices)), "sector")
        price_index = (root_sum / sectors_all) ** 2
        relative = prices / price_index
        continuation = jnp.where(live, jnp.maximum(values, scrap), scrap)
        expect = jnp.einsum(
            "zw,swk->szk", transition, continuation, precision=lax.Precision.HIGHEST
        )
        forward_value = 0.9 * expect - install_cost[None, None, :]
        empty = jnp.full((sec_dev * prod_count, cap_dev), -1e30, jnp.float32)
        shard_cols = lax.all_gather(forward_value, "cap", axis=2, tiled=True)
        best = jnp.maximum(
            empty,
            best_reply(
                shard_cols.reshape(sec_dev * prod_count, shard_cols.shape[2]), row_first, cap_dev
            ),
        ).reshape(sec_dev, prod_count, cap_dev)
        values = jnp.where(live, relative[:, None, None] * output + best, scrap)
    return (values, relative)


def running_max(arr, lane, backward):
    width = arr.shape[1]

    def shifted(part, step):
        if backward:
            return jnp.where(lane < width - step, pltpu.roll(part, width - step, 1), NEG)
        return jnp.where(lane >= step, pltpu.roll(part, step, 1), NEG)

    arr = shifted(arr, 1)
    step = 1
    while step < width:
        arr = jnp.maximum(arr, shifted(arr, step))
        step *= 2
    return arr


def undominated(gain, square, t_low, t_high, lane):
    low = gain - square * t_low
    high = gain - square * t_high
    return (low > running_max(low, lane, False)) & (high > running_max(high, lane, True))


def compress(keep, before, lane, gain):
    width = gain.shape[1]
    shift = jnp.where(keep, lane - before, 0)
    gain = jnp.where(keep, gain, NEG)
    left = shift
    step = 1
    while step < width:
        move_gain = pltpu.roll(gain, width - step, 1)
        move_left = pltpu.roll(left, width - step, 1)
        arrive = (move_left & step) != 0
        leave = (left & step) != 0
        gain = jnp.where(arrive, move_gain, jnp.where(leave, NEG, gain))
        left = jnp.where(arrive, move_left, jnp.where(leave, 0, left))
        step *= 2
    return gain, left


def sweeps_kernel(n_sec, n_cap, start_ref, mass_ref, survive_ref, exit_ref, demand_ref, trans_ref, cost_ref,
                  value_ref, rel_ref, flag_ref,
                  out_ref, forward_ref, tri_ref, wide_ref, over_ref, part_ref, parts_ref, pay_ref, pays_ref,
                  root_ref, roots_ref, part_send, part_recv, pay_send, pay_recv, root_send, root_recv):
    sec_dev, prods, cap_dev = start_ref.shape
    total = cap_dev * n_cap
    me_cap = lax.axis_index("cap")
    me_sec = lax.axis_index("sector")
    mesh_id = pl.DeviceIdType.MESH

    barrier = pltpu.get_barrier_semaphore()
    for off in range(1, n_cap):
        pl.semaphore_signal(barrier, inc=1, device_id={"cap": lax.rem(me_cap + off, n_cap)}, device_id_type=mesh_id)
    for off in range(1, n_sec):
        pl.semaphore_signal(barrier, inc=1, device_id={"sector": lax.rem(me_sec + off, n_sec)}, device_id_type=mesh_id)

    lane = lax.broadcasted_iota(jnp.int32, (prods, cap_dev), 1)
    lane_one = lax.broadcasted_iota(jnp.int32, (1, cap_dev), 1)
    lane_tile = lax.broadcasted_iota(jnp.int32, (prods, 128), 1)
    prod_col = lax.broadcasted_iota(jnp.int32, (prods, cap_dev), 0)
    first = me_cap * cap_dev
    capital = capital_of(first + lane_one, total)
    slope = 1.0 / capital
    scrap = 0.3 * capital
    power = jnp.exp(0.6 * (math.log(0.2) + math.log(10.0) * (first + lane_one).astype(jnp.float32) / (total - 1)))
    out_ref[...] = jnp.exp(-0.5 + prod_col.astype(jnp.float32) / (prods - 1)) * power
    tri_ref[...] = (
        lax.broadcasted_iota(jnp.int32, (cap_dev, cap_dev), 0) < lax.broadcasted_iota(jnp.int32, (cap_dev, cap_dev), 1)
    ).astype(jnp.bfloat16)
    t_low, t_high = 1.0 / 2.0, 1.0 / 0.2
    halves = sec_dev // 4
    over_ref[...] = jnp.zeros_like(over_ref)

    def live_of(s):
        return (survive_ref[s] == 1) & (prod_col >= exit_ref[s])

    copies = []
    pl.semaphore_wait(barrier, n_cap - 1 + n_sec - 1)
    for sweep in range(SWEEPS):
        source = start_ref if sweep == 0 else value_ref

        def supply_step(s, carry):
            stay = jax.nn.sigmoid((source[s] - scrap) / 0.5)
            weighted = jnp.where(live_of(s), mass_ref[s] * stay * out_ref[...], 0.0)
            row = jnp.sum(weighted, axis=0, keepdims=True)
            folded = row[:, 0:128]
            for at in range(128, cap_dev, 128):
                folded = folded + row[:, at:at + 128]
            part_ref[sweep, pl.ds(s, 1), :] = folded
            return carry

        lax.fori_loop(0, sec_dev, supply_step, 0)
        part_copies = []
        for off in range(1, n_cap):
            part_copies.append(pltpu.make_async_remote_copy(
                src_ref=part_ref.at[sweep], dst_ref=parts_ref.at[sweep, me_cap],
                send_sem=part_send.at[sweep, off - 1], recv_sem=part_recv.at[sweep, off - 1],
                device_id={"cap": lax.rem(me_cap + off, n_cap)}, device_id_type=mesh_id))
            part_copies[-1].start()
        parts_ref[sweep, me_cap] = part_ref[sweep]

        pay_ref[sweep] = jnp.full(pay_ref.shape[1:], NEG, jnp.float32)

        def forward_step(s, carry):
            vals = source[s]
            cont = jnp.where(live_of(s), jnp.maximum(vals, scrap), scrap)
            expect = jnp.dot(trans_ref[...], cont, precision=lax.Precision.HIGHEST, preferred_element_type=jnp.float32)
            forward = 0.9 * expect - cost_ref[...]
            forward_ref[s] = forward
            gain = forward + 0.8 * capital
            keep = undominated(gain, capital * capital, t_low, t_high, lane)
            before = jnp.dot(keep.astype(jnp.bfloat16), tri_ref[...], preferred_element_type=jnp.float32)
            packed, moved = compress(keep, before.astype(jnp.int32), lane, gain)
            packed, moved = packed[:, 0:128], moved[:, 0:128]
            over_ref[...] = jnp.maximum(over_ref[...], jnp.where((lane_tile == SLOTS) & (packed > 0.5 * NEG), 1.0, 0.0))
            square = capital_of(first + lane_tile + moved, total)
            square = jnp.where(packed > 0.5 * NEG, square * square, 0.0)
            both = jnp.where(lane_tile < SLOTS, packed, pltpu.roll(square, SLOTS, 1))
            group = s // halves
            rows = pl.ds(pl.multiple_of((s % halves) * prods, prods), prods)
            placed = pltpu.roll(both, group * (2 * SLOTS), 1)
            pay_ref[sweep, rows, :] = jnp.where(lane_tile // (2 * SLOTS) == group, placed, pay_ref[sweep, rows, :])
            return carry

        lax.fori_loop(0, sec_dev, forward_step, 0)
        flags = over_ref[0:8, :]
        for at in range(8, prods, 8):
            flags = jnp.maximum(flags, over_ref[at:at + 8, :])
        pay_ref[sweep, halves * prods:halves * prods + 8, :] = flags
        pay_copies = []
        for off in range(1, n_cap):
            pay_copies.append(pltpu.make_async_remote_copy(
                src_ref=pay_ref.at[sweep], dst_ref=pays_ref.at[sweep, me_cap],
                send_sem=pay_send.at[sweep, off - 1], recv_sem=pay_recv.at[sweep, off - 1],
                device_id={"cap": lax.rem(me_cap + off, n_cap)}, device_id_type=mesh_id))
            pay_copies[-1].start()
        pays_ref[sweep, me_cap] = pay_ref[sweep]

        for copy in part_copies:
            copy.wait_recv()
        gathered = parts_ref[sweep, 0]
        for d in range(1, n_cap):
            gathered = gathered + parts_ref[sweep, d]
        supply = 1.0 + jnp.sum(gathered, axis=1, keepdims=True) / (prods * total)
        prices = jnp.sqrt(demand_ref[...] / supply)
        for copy in pay_copies:
            copy.wait_recv()
        flag_rows = pl.ds(halves * prods, 8)
        flags = pays_ref[sweep, 0, flag_rows, :]
        for d in range(1, n_cap):
            flags = jnp.maximum(flags, pays_ref[sweep, d, flag_rows, :])
        root_ref[sweep, 0:sec_dev, :] = jnp.broadcast_to(jnp.sqrt(prices), (sec_dev, 128))
        root_ref[sweep, sec_dev:sec_dev + 8, :] = flags
        root_copies = []
        for off in range(1, n_sec):
            root_copies.append(pltpu.make_async_remote_copy(
                src_ref=root_ref.at[sweep], dst_ref=roots_ref.at[sweep, me_sec],
                send_sem=root_send.at[sweep, off - 1], recv_sem=root_recv.at[sweep, off - 1],
                device_id={"sector": lax.rem(me_sec + off, n_sec)}, device_id_type=mesh_id))
            root_copies[-1].start()
        roots_ref[sweep, me_sec] = root_ref[sweep]

        def best_step(s, carry):
            group = s // halves
            rows = pl.ds(pl.multiple_of((s % halves) * prods, prods), prods)
            best = jnp.full((prods, cap_dev), NEG, jnp.float32)
            for d in range(n_cap):
                block = pltpu.roll(pays_ref[sweep, d, rows, :], lax.rem(128 - group * (2 * SLOTS), 128), 1)
                for c in range(SLOTS):
                    best = jnp.maximum(best, block[:, c:c + 1] - block[:, SLOTS + c:SLOTS + c + 1] * slope)
            forward_ref[s] = jnp.maximum(best - 1.41 * capital, forward_ref[s] - 0.11 * capital)
            return carry

        lax.fori_loop(0, sec_dev, best_step, 0)

        for copy in root_copies:
            copy.wait_recv()
        root_sum = roots_ref[sweep, 0]
        for d in range(1, n_sec):
            root_sum = root_sum + roots_ref[sweep, d]
        mean = jnp.sum(root_sum[0:sec_dev], axis=0, keepdims=True) / (sec_dev * n_sec)
        relative = prices / (mean[:, 0:1] * mean[:, 0:1])
        wide_ref[...] = jnp.broadcast_to(relative, (sec_dev, cap_dev))

        def value_step(s, carry):
            value_ref[s] = jnp.where(live_of(s), wide_ref[pl.ds(s, 1), :] * out_ref[...] + forward_ref[s], scrap)
            return carry

        lax.fori_loop(0, sec_dev, value_step, 0)
        copies += part_copies + pay_copies + root_copies
    rel_ref[...] = jnp.broadcast_to(relative, (sec_dev, 128))
    flag_ref[...] = root_sum[sec_dev:sec_dev + 8]
    for copy in copies:
        copy.wait_send()


def pruned_sweeps(start_value, firm_mass, survive, exit_index, demand, transition, install_cost):
    n_sec, n_cap = lax.axis_size("sector"), lax.axis_size("cap")
    sec_dev, prods, cap_dev = start_value.shape
    pay_rows = sec_dev // 4 * prods + 8
    vmem = pl.BlockSpec(memory_space=pltpu.VMEM)
    smem = pl.BlockSpec(memory_space=pltpu.SMEM)
    f32 = jnp.float32
    return pl.pallas_call(
        functools.partial(sweeps_kernel, n_sec, n_cap),
        out_shape=(
            jax.ShapeDtypeStruct(start_value.shape, f32),
            jax.ShapeDtypeStruct((sec_dev, 128), f32),
            jax.ShapeDtypeStruct((8, 128), f32),
        ),
        in_specs=[vmem, vmem, vmem, smem, vmem, vmem, vmem],
        out_specs=(vmem, vmem, vmem),
        scratch_shapes=[
            pltpu.VMEM((prods, cap_dev), f32),
            pltpu.VMEM(start_value.shape, f32),
            pltpu.VMEM((cap_dev, cap_dev), jnp.bfloat16),
            pltpu.VMEM((sec_dev, cap_dev), f32),
            pltpu.VMEM((prods, 128), f32),
            pltpu.VMEM((SWEEPS, sec_dev, 128), f32),
            pltpu.VMEM((SWEEPS, n_cap, sec_dev, 128), f32),
            pltpu.VMEM((SWEEPS, pay_rows, 128), f32),
            pltpu.VMEM((SWEEPS, n_cap, pay_rows, 128), f32),
            pltpu.VMEM((SWEEPS, sec_dev + 8, 128), f32),
            pltpu.VMEM((SWEEPS, n_sec, sec_dev + 8, 128), f32),
            pltpu.SemaphoreType.DMA((SWEEPS, n_cap - 1)),
            pltpu.SemaphoreType.DMA((SWEEPS, n_cap - 1)),
            pltpu.SemaphoreType.DMA((SWEEPS, n_cap - 1)),
            pltpu.SemaphoreType.DMA((SWEEPS, n_cap - 1)),
            pltpu.SemaphoreType.DMA((SWEEPS, n_sec - 1)),
            pltpu.SemaphoreType.DMA((SWEEPS, n_sec - 1)),
        ],
        compiler_params=pltpu.CompilerParams(
            collective_id=0, has_side_effects=True, vmem_limit_bytes=48 * 1024 * 1024
        ),
    )(start_value, firm_mass, survive, exit_index, demand[:, None], transition, install_cost[None, :])


def on_device(start_value, firm_mass, survive, exit_index, demand, transition, install_cost):
    args = (start_value, firm_mass, survive, exit_index, demand, transition, install_cost)
    sec_dev, prods, cap_dev = start_value.shape
    if sec_dev % 8 or prods % 8 or cap_dev % 128 or min(lax.axis_size("sector"), lax.axis_size("cap")) < 2:
        return dense_sweeps(*args)
    values, relative, flags = pruned_sweeps(*args)
    return lax.cond(
        jnp.max(flags) > 0.0,
        lambda: dense_sweeps(*args),
        lambda: (values, relative[:, 0]),
    )


def solution(mesh):
    return jax.shard_map(
        on_device,
        mesh=mesh,
        in_specs=(
            P("sector", None, "cap"),
            P("sector", None, "cap"),
            P("sector", None, "cap"),
            P("sector"),
            P("sector"),
            P(),
            P("cap"),
        ),
        out_specs=(P("sector", None, "cap"), P("sector")),
        check_vma=False,
    )
```

```python
import functools
import math

import jax
import jax.numpy as jnp
from jax import lax
from jax.experimental import pallas as pl
from jax.experimental.pallas import tpu as pltpu
from jax.sharding import PartitionSpec as P

SWEEPS = 2
SLOTS = 16
OWN_SLOTS = 16
NEG = -1e30


def capital_of(positions, total):
    return 0.2 * jnp.exp(math.log(10.0) * positions.astype(jnp.float32) / (total - 1))


def charge_of(cap_now, cap_next, row_ids, col_ids):
    invest = cap_next - 0.9 * cap_now
    fixed = jnp.where(row_ids == col_ids, 0.0, 1.5 * cap_now)
    return invest + invest * invest / cap_now + fixed


def best_reply(forward_rows, row_first, row_count):
    total_rows, total_cols = forward_rows.shape
    cap_of = functools.partial(capital_of, total=total_cols)
    col_block = math.gcd(total_cols, 2048)
    row_block = math.gcd(row_count, 512)
    grp_limit = max(1, (1 << 24) // (row_block * col_block))
    grp_size = math.gcd(total_rows, 1 << min(total_rows, grp_limit).bit_length() - 1)
    groups = forward_rows.reshape(total_rows // grp_size, grp_size, total_cols)

    def one_group(group):
        row_ids = row_first + 0 * row_block + jnp.arange(row_block, dtype=jnp.int32)
        cap_rows = cap_of(row_ids)
        empty = jnp.full((grp_size, row_block), -1e30, jnp.float32)
        col_ids = jnp.arange(col_block, dtype=jnp.int32)
        cap_cols = cap_of(col_ids)
        charge = charge_of(cap_rows[:, None], cap_cols[None, :], row_ids[:, None], col_ids[None, :])
        return jnp.maximum(empty, jnp.max(group[:, None, :] - charge[None], axis=2))

    return lax.map(one_group, groups).reshape(total_rows, row_count)


def dense_sweeps(start_value, firm_mass, survive, exit_index, demand, transition, install_cost):
    sec_dev, prod_count, cap_dev = start_value.shape
    sectors_all = sec_dev * lax.axis_size("sector")
    row_first = lax.axis_index("cap") * cap_dev
    prod_index = jnp.arange(prod_count, dtype=jnp.int32)
    total = cap_dev * lax.axis_size("cap")
    capital = capital_of(row_first + jnp.arange(cap_dev, dtype=jnp.int32), total)
    log_prod = -0.5 + prod_index.astype(jnp.float32) / (prod_count - 1)
    output = jnp.exp(log_prod)[:, None] * capital[None, :] ** 0.6
    scrap = 0.3 * capital
    live = (survive == 1) & (prod_index[None, :, None] >= exit_index[:, None, None])
    values = start_value
    relative = jnp.zeros((sec_dev,), jnp.float32)
    for sweep in range(SWEEPS):
        staying = jnp.where(live, jax.nn.sigmoid((values - scrap) / 0.5), 0.0)
        partial_value = jnp.sum(firm_mass * staying * output, axis=(1, 2))
        supply = 1.0 + lax.psum(partial_value, "cap") / (prod_count * total)
        prices = jnp.sqrt(demand / supply)
        root_sum = lax.psum(jnp.sum(jnp.sqrt(prices)), "sector")
        price_index = (root_sum / sectors_all) ** 2
        relative = prices / price_index
        continuation = jnp.where(live, jnp.maximum(values, scrap), scrap)
        expect = jnp.einsum(
            "zw,swk->szk", transition, continuation, precision=lax.Precision.HIGHEST
        )
        forward_value = 0.9 * expect - install_cost[None, None, :]
        empty = jnp.full((sec_dev * prod_count, cap_dev), -1e30, jnp.float32)
        shard_cols = lax.all_gather(forward_value, "cap", axis=2, tiled=True)
        best = jnp.maximum(
            empty,
            best_reply(
                shard_cols.reshape(sec_dev * prod_count, shard_cols.shape[2]), row_first, cap_dev
            ),
        ).reshape(sec_dev, prod_count, cap_dev)
        values = jnp.where(live, relative[:, None, None] * output + best, scrap)
    return (values, relative)


def running_max(arr, lane, backward):
    width = arr.shape[1]

    def shifted(part, step):
        if backward:
            return jnp.where(lane < width - step, pltpu.roll(part, width - step, 1), NEG)
        return jnp.where(lane >= step, pltpu.roll(part, step, 1), NEG)

    arr = shifted(arr, 1)
    step = 1
    while step < width:
        arr = jnp.maximum(arr, shifted(arr, step))
        step *= 2
    return arr


def undominated(gain, square, t_low, t_high, lane):
    low = gain - square * t_low
    high = gain - square * t_high
    return (low > running_max(low, lane, False)) & (high > running_max(high, lane, True))


def compress(keep, before, lane, gain, extra=None):
    width = gain.shape[1]
    shift = jnp.where(keep, lane - before, 0)
    gain = jnp.where(keep, gain, NEG)
    left = shift
    step = 1
    while step < width:
        move_gain = pltpu.roll(gain, width - step, 1)
        move_left = pltpu.roll(left, width - step, 1)
        arrive = (move_left & step) != 0
        leave = (left & step) != 0
        gain = jnp.where(arrive, move_gain, jnp.where(leave, NEG, gain))
        if extra is not None:
            extra = jnp.where(arrive, pltpu.roll(extra, width - step, 1), extra)
        left = jnp.where(arrive, move_left, jnp.where(leave, 0, left))
        step *= 2
    return gain, left if extra is None else extra


def sweeps_kernel(n_sec, n_cap, start_ref, mass_ref, survive_ref, exit_ref, demand_ref, trans_ref, cost_ref,
                  value_ref, rel_ref, flag_ref,
                  out_ref, forward_ref, tri_ref, wide_ref, over_ref, part_ref, parts_ref, pay_ref, pays_ref,
                  root_ref, roots_ref, mark_ref, marks_ref, best_ref, mark_send, mark_recv, part_send, part_recv, pay_send, pay_recv, root_send, root_recv):
    sec_dev, prods, cap_dev = start_ref.shape
    total = cap_dev * n_cap
    me_cap = lax.axis_index("cap")
    me_sec = lax.axis_index("sector")
    mesh_id = pl.DeviceIdType.MESH

    barrier = pltpu.get_barrier_semaphore()
    for off in range(1, n_cap):
        pl.semaphore_signal(barrier, inc=1, device_id={"cap": lax.rem(me_cap + off, n_cap)}, device_id_type=mesh_id)
    for off in range(1, n_sec):
        pl.semaphore_signal(barrier, inc=1, device_id={"sector": lax.rem(me_sec + off, n_sec)}, device_id_type=mesh_id)

    lane = lax.broadcasted_iota(jnp.int32, (prods, cap_dev), 1)
    lane_one = lax.broadcasted_iota(jnp.int32, (1, cap_dev), 1)
    lane_tile = lax.broadcasted_iota(jnp.int32, (prods, 128), 1)
    prod_col = lax.broadcasted_iota(jnp.int32, (prods, cap_dev), 0)
    first = me_cap * cap_dev
    capital = capital_of(first + lane_one, total)
    slope = 1.0 / capital
    scrap = 0.3 * capital
    power = jnp.exp(0.6 * (math.log(0.2) + math.log(10.0) * (first + lane_one).astype(jnp.float32) / (total - 1)))
    out_ref[...] = jnp.exp(-0.5 + prod_col.astype(jnp.float32) / (prods - 1)) * power
    tri_ref[...] = (
        lax.broadcasted_iota(jnp.int32, tri_ref.shape, 0) < lax.broadcasted_iota(jnp.int32, tri_ref.shape, 1)
    ).astype(jnp.bfloat16)
    t_low, t_high = 1.0 / 2.0, 1.0 / 0.2
    halves = sec_dev // 4
    merged_width = 128 * pl.cdiv(n_cap, 4)
    lane_merged = lax.broadcasted_iota(jnp.int32, (prods, merged_width), 1)
    own_low = jnp.broadcast_to(slope[:, cap_dev - 1:cap_dev], (prods, merged_width))
    own_high = jnp.broadcast_to(slope[:, 0:1], (prods, merged_width))
    over_ref[...] = jnp.zeros_like(over_ref)

    def live_of(s):
        return (survive_ref[s] == 1) & (prod_col >= exit_ref[s])

    copies = []
    pl.semaphore_wait(barrier, n_cap - 1 + n_sec - 1)
    for sweep in range(SWEEPS):
        source = start_ref if sweep == 0 else value_ref

        def supply_step(s, carry):
            stay = jax.nn.sigmoid((source[s] - scrap) / 0.5)
            weighted = jnp.where(live_of(s), mass_ref[s] * stay * out_ref[...], 0.0)
            row = jnp.sum(weighted, axis=0, keepdims=True)
            folded = row[:, 0:128]
            for at in range(128, cap_dev, 128):
                folded = folded + row[:, at:at + 128]
            part_ref[sweep, pl.ds(s, 1), :] = folded
            return carry

        lax.fori_loop(0, sec_dev, supply_step, 0)
        part_copies = []
        for off in range(1, n_cap):
            part_copies.append(pltpu.make_async_remote_copy(
                src_ref=part_ref.at[sweep], dst_ref=parts_ref.at[sweep, me_cap],
                send_sem=part_send.at[sweep, off - 1], recv_sem=part_recv.at[sweep, off - 1],
                device_id={"cap": lax.rem(me_cap + off, n_cap)}, device_id_type=mesh_id))
            part_copies[-1].start()
        parts_ref[sweep, me_cap] = part_ref[sweep]

        pay_ref[sweep] = jnp.full(pay_ref.shape[1:], NEG, jnp.float32)

        def forward_step(s, carry):
            vals = source[s]
            cont = jnp.where(live_of(s), jnp.maximum(vals, scrap), scrap)
            expect = jnp.dot(trans_ref[...], cont, precision=lax.Precision.HIGHEST, preferred_element_type=jnp.float32)
            forward = 0.9 * expect - cost_ref[...]
            forward_ref[s] = forward
            gain = forward + 0.8 * capital
            keep = undominated(gain, capital * capital, t_low, t_high, lane)
            before = jnp.dot(keep.astype(jnp.bfloat16), tri_ref[0:cap_dev, 0:cap_dev], preferred_element_type=jnp.float32)
            packed, moved = compress(keep, before.astype(jnp.int32), lane, gain)
            packed, moved = packed[:, 0:128], moved[:, 0:128]
            over_ref[...] = jnp.maximum(over_ref[...], jnp.where((lane_tile == SLOTS) & (packed > 0.5 * NEG), 1.0, 0.0))
            square = capital_of(first + lane_tile + moved, total)
            square = jnp.where(packed > 0.5 * NEG, square * square, 0.0)
            both = jnp.where(lane_tile < SLOTS, packed, pltpu.roll(square, SLOTS, 1))
            group = s // halves
            rows = pl.ds(pl.multiple_of((s % halves) * prods, prods), prods)
            placed = pltpu.roll(both, group * (2 * SLOTS), 1)
            pay_ref[sweep, rows, :] = jnp.where(lane_tile // (2 * SLOTS) == group, placed, pay_ref[sweep, rows, :])
            return carry

        def flags_so_far():
            flags = over_ref[0:8, :]
            for at in range(8, prods, 8):
                flags = jnp.maximum(flags, over_ref[at:at + 8, :])
            return flags

        lax.fori_loop(0, sec_dev, forward_step, 0)
        flags = flags_so_far()
        pay_ref[sweep, halves * prods:halves * prods + 8, :] = flags
        pay_copies = []
        for off in range(1, n_cap):
            pay_copies.append(pltpu.make_async_remote_copy(
                src_ref=pay_ref.at[sweep], dst_ref=pays_ref.at[sweep, me_cap],
                send_sem=pay_send.at[sweep, off - 1], recv_sem=pay_recv.at[sweep, off - 1],
                device_id={"cap": lax.rem(me_cap + off, n_cap)}, device_id_type=mesh_id))
            pay_copies[-1].start()
        pays_ref[sweep, me_cap] = pay_ref[sweep]

        for copy in part_copies:
            copy.wait_recv()
        gathered = parts_ref[sweep, 0]
        for d in range(1, n_cap):
            gathered = gathered + parts_ref[sweep, d]
        supply = 1.0 + jnp.sum(gathered, axis=1, keepdims=True) / (prods * total)
        prices = jnp.sqrt(demand_ref[...] / supply)
        for copy in pay_copies:
            copy.wait_recv()
        flag_rows = pl.ds(halves * prods, 8)
        flags = pays_ref[sweep, 0, flag_rows, :]
        for d in range(1, n_cap):
            flags = jnp.maximum(flags, pays_ref[sweep, d, flag_rows, :])

        def select_step(s, carry):
            group = s // halves
            rows = pl.ds(pl.multiple_of((s % halves) * prods, prods), prods)
            tiles = []
            for d in range(n_cap):
                block = pltpu.roll(pays_ref[sweep, d, rows, :], lax.rem((d % 4) * (2 * SLOTS) + 128 - group * (2 * SLOTS), 128), 1)
                if d % 4 == 0:
                    tiles.append(jnp.where(lane_tile < 2 * SLOTS, block, NEG))
                else:
                    tiles[-1] = jnp.where(lane_tile // (2 * SLOTS) == d % 4, block, tiles[-1])
            merged = tiles[0] if len(tiles) == 1 else jnp.concatenate(tiles, axis=1)
            gain = jnp.where(lane_merged % (2 * SLOTS) < SLOTS, merged, NEG)
            square = jnp.where(gain > 0.5 * NEG, pltpu.roll(merged, merged_width - SLOTS, 1), 0.0)
            keep = undominated(gain, square, own_low, own_high, lane_merged) & (gain > 0.5 * NEG)
            before = jnp.dot(keep.astype(jnp.bfloat16), tri_ref[0:merged_width, 0:merged_width], preferred_element_type=jnp.float32)
            packed, square = compress(keep, before.astype(jnp.int32), lane_merged, gain, square)
            packed, square = packed[:, 0:128], square[:, 0:128]
            over_ref[...] = jnp.maximum(over_ref[...], jnp.where((lane_tile == OWN_SLOTS) & (packed > 0.5 * NEG), 1.0, 0.0))
            best_ref[s] = jnp.where(lane_tile < OWN_SLOTS, packed, pltpu.roll(square, OWN_SLOTS, 1))
            return carry

        def best_step(s, carry):
            block = best_ref[s]
            best = jnp.full((prods, cap_dev), NEG, jnp.float32)
            for c in range(OWN_SLOTS):
                best = jnp.maximum(best, block[:, c:c + 1] - block[:, OWN_SLOTS + c:OWN_SLOTS + c + 1] * slope)
            forward_ref[s] = jnp.maximum(best - 1.41 * capital, forward_ref[s] - 0.11 * capital)
            return carry

        mark_copies = []
        if sweep == SWEEPS - 1:
            lax.fori_loop(0, sec_dev, select_step, 0)
            mark_ref[...] = jnp.maximum(flags, flags_so_far())
            for off in range(1, n_cap):
                mark_copies.append(pltpu.make_async_remote_copy(
                    src_ref=mark_ref, dst_ref=marks_ref.at[me_cap],
                    send_sem=mark_send.at[off - 1], recv_sem=mark_recv.at[off - 1],
                    device_id={"cap": lax.rem(me_cap + off, n_cap)}, device_id_type=mesh_id))
                mark_copies[-1].start()
            marks_ref[me_cap] = mark_ref[...]
            lax.fori_loop(0, sec_dev, best_step, 0)
            for copy in mark_copies:
                copy.wait_recv()
            for d in range(n_cap):
                flags = jnp.maximum(flags, marks_ref[d])

        root_ref[sweep, 0:sec_dev, :] = jnp.broadcast_to(jnp.sqrt(prices), (sec_dev, 128))
        root_ref[sweep, sec_dev:sec_dev + 8, :] = flags
        root_copies = []
        for off in range(1, n_sec):
            root_copies.append(pltpu.make_async_remote_copy(
                src_ref=root_ref.at[sweep], dst_ref=roots_ref.at[sweep, me_sec],
                send_sem=root_send.at[sweep, off - 1], recv_sem=root_recv.at[sweep, off - 1],
                device_id={"sector": lax.rem(me_sec + off, n_sec)}, device_id_type=mesh_id))
            root_copies[-1].start()
        roots_ref[sweep, me_sec] = root_ref[sweep]

        if sweep < SWEEPS - 1:
            lax.fori_loop(0, sec_dev, select_step, 0)
            lax.fori_loop(0, sec_dev, best_step, 0)

        for copy in root_copies:
            copy.wait_recv()
        root_sum = roots_ref[sweep, 0]
        for d in range(1, n_sec):
            root_sum = root_sum + roots_ref[sweep, d]
        mean = jnp.sum(root_sum[0:sec_dev], axis=0, keepdims=True) / (sec_dev * n_sec)
        relative = prices / (mean[:, 0:1] * mean[:, 0:1])
        wide_ref[...] = jnp.broadcast_to(relative, (sec_dev, cap_dev))

        def value_step(s, carry):
            value_ref[s] = jnp.where(live_of(s), wide_ref[pl.ds(s, 1), :] * out_ref[...] + forward_ref[s], scrap)
            return carry

        lax.fori_loop(0, sec_dev, value_step, 0)
        copies += part_copies + pay_copies + root_copies + mark_copies
    rel_ref[...] = jnp.broadcast_to(relative, (sec_dev, 128))
    flag_ref[...] = root_sum[sec_dev:sec_dev + 8]
    for copy in copies:
        copy.wait_send()


def pruned_sweeps(start_value, firm_mass, survive, exit_index, demand, transition, install_cost):
    n_sec, n_cap = lax.axis_size("sector"), lax.axis_size("cap")
    sec_dev, prods, cap_dev = start_value.shape
    pay_rows = sec_dev // 4 * prods + 8
    merged_width = 128 * pl.cdiv(n_cap, 4)
    vmem = pl.BlockSpec(memory_space=pltpu.VMEM)
    smem = pl.BlockSpec(memory_space=pltpu.SMEM)
    f32 = jnp.float32
    return pl.pallas_call(
        functools.partial(sweeps_kernel, n_sec, n_cap),
        out_shape=(
            jax.ShapeDtypeStruct(start_value.shape, f32),
            jax.ShapeDtypeStruct((sec_dev, 128), f32),
            jax.ShapeDtypeStruct((8, 128), f32),
        ),
        in_specs=[vmem, vmem, vmem, smem, vmem, vmem, vmem],
        out_specs=(vmem, vmem, vmem),
        scratch_shapes=[
            pltpu.VMEM((prods, cap_dev), f32),
            pltpu.VMEM(start_value.shape, f32),
            pltpu.VMEM((max(cap_dev, merged_width),) * 2, jnp.bfloat16),
            pltpu.VMEM((sec_dev, cap_dev), f32),
            pltpu.VMEM((prods, 128), f32),
            pltpu.VMEM((SWEEPS, sec_dev, 128), f32),
            pltpu.VMEM((SWEEPS, n_cap, sec_dev, 128), f32),
            pltpu.VMEM((SWEEPS, pay_rows, 128), f32),
            pltpu.VMEM((SWEEPS, n_cap, pay_rows, 128), f32),
            pltpu.VMEM((SWEEPS, sec_dev + 8, 128), f32),
            pltpu.VMEM((SWEEPS, n_sec, sec_dev + 8, 128), f32),
            pltpu.VMEM((8, 128), f32),
            pltpu.VMEM((n_cap, 8, 128), f32),
            pltpu.VMEM((sec_dev, prods, 128), f32),
            pltpu.SemaphoreType.DMA((n_cap - 1,)),
            pltpu.SemaphoreType.DMA((n_cap - 1,)),
            pltpu.SemaphoreType.DMA((SWEEPS, n_cap - 1)),
            pltpu.SemaphoreType.DMA((SWEEPS, n_cap - 1)),
            pltpu.SemaphoreType.DMA((SWEEPS, n_cap - 1)),
            pltpu.SemaphoreType.DMA((SWEEPS, n_cap - 1)),
            pltpu.SemaphoreType.DMA((SWEEPS, n_sec - 1)),
            pltpu.SemaphoreType.DMA((SWEEPS, n_sec - 1)),
        ],
        compiler_params=pltpu.CompilerParams(
            collective_id=0, has_side_effects=True, vmem_limit_bytes=48 * 1024 * 1024
        ),
    )(start_value, firm_mass, survive, exit_index, demand[:, None], transition, install_cost[None, :])


def on_device(start_value, firm_mass, survive, exit_index, demand, transition, install_cost):
    args = (start_value, firm_mass, survive, exit_index, demand, transition, install_cost)
    sec_dev, prods, cap_dev = start_value.shape
    if sec_dev % 8 or prods % 8 or cap_dev % 128 or min(lax.axis_size("sector"), lax.axis_size("cap")) < 2:
        return dense_sweeps(*args)
    values, relative, flags = pruned_sweeps(*args)
    return lax.cond(
        jnp.max(flags) > 0.0,
        lambda: dense_sweeps(*args),
        lambda: (values, relative[:, 0]),
    )


def solution(mesh):
    return jax.shard_map(
        on_device,
        mesh=mesh,
        in_specs=(
            P("sector", None, "cap"),
            P("sector", None, "cap"),
            P("sector", None, "cap"),
            P("sector"),
            P("sector"),
            P(),
            P("cap"),
        ),
        out_specs=(P("sector", None, "cap"), P("sector")),
        check_vma=False,
    )
```

```python
import functools
import math

import jax
import jax.numpy as jnp
from jax import lax
from jax.experimental import pallas as pl
from jax.experimental.pallas import tpu as pltpu
from jax.sharding import PartitionSpec as P

SWEEPS = 2
SLOTS = 16
OWN_SLOTS = 16
NEG = -1e30


def capital_of(positions, total):
    return 0.2 * jnp.exp(math.log(10.0) * positions.astype(jnp.float32) / (total - 1))


def charge_of(cap_now, cap_next, row_ids, col_ids):
    invest = cap_next - 0.9 * cap_now
    fixed = jnp.where(row_ids == col_ids, 0.0, 1.5 * cap_now)
    return invest + invest * invest / cap_now + fixed


def best_reply(forward_rows, row_first, row_count):
    total_rows, total_cols = forward_rows.shape
    cap_of = functools.partial(capital_of, total=total_cols)
    col_block = math.gcd(total_cols, 2048)
    row_block = math.gcd(row_count, 512)
    grp_limit = max(1, (1 << 24) // (row_block * col_block))
    grp_size = math.gcd(total_rows, 1 << min(total_rows, grp_limit).bit_length() - 1)
    groups = forward_rows.reshape(total_rows // grp_size, grp_size, total_cols)

    def one_group(group):
        row_ids = row_first + 0 * row_block + jnp.arange(row_block, dtype=jnp.int32)
        cap_rows = cap_of(row_ids)
        empty = jnp.full((grp_size, row_block), -1e30, jnp.float32)
        col_ids = jnp.arange(col_block, dtype=jnp.int32)
        cap_cols = cap_of(col_ids)
        charge = charge_of(cap_rows[:, None], cap_cols[None, :], row_ids[:, None], col_ids[None, :])
        return jnp.maximum(empty, jnp.max(group[:, None, :] - charge[None], axis=2))

    return lax.map(one_group, groups).reshape(total_rows, row_count)


def dense_sweeps(start_value, firm_mass, survive, exit_index, demand, transition, install_cost):
    sec_dev, prod_count, cap_dev = start_value.shape
    sectors_all = sec_dev * lax.axis_size("sector")
    row_first = lax.axis_index("cap") * cap_dev
    prod_index = jnp.arange(prod_count, dtype=jnp.int32)
    total = cap_dev * lax.axis_size("cap")
    capital = capital_of(row_first + jnp.arange(cap_dev, dtype=jnp.int32), total)
    log_prod = -0.5 + prod_index.astype(jnp.float32) / (prod_count - 1)
    output = jnp.exp(log_prod)[:, None] * capital[None, :] ** 0.6
    scrap = 0.3 * capital
    live = (survive == 1) & (prod_index[None, :, None] >= exit_index[:, None, None])
    values = start_value
    relative = jnp.zeros((sec_dev,), jnp.float32)
    for sweep in range(SWEEPS):
        staying = jnp.where(live, jax.nn.sigmoid((values - scrap) / 0.5), 0.0)
        partial_value = jnp.sum(firm_mass * staying * output, axis=(1, 2))
        supply = 1.0 + lax.psum(partial_value, "cap") / (prod_count * total)
        prices = jnp.sqrt(demand / supply)
        root_sum = lax.psum(jnp.sum(jnp.sqrt(prices)), "sector")
        price_index = (root_sum / sectors_all) ** 2
        relative = prices / price_index
        continuation = jnp.where(live, jnp.maximum(values, scrap), scrap)
        expect = jnp.einsum(
            "zw,swk->szk", transition, continuation, precision=lax.Precision.HIGHEST
        )
        forward_value = 0.9 * expect - install_cost[None, None, :]
        empty = jnp.full((sec_dev * prod_count, cap_dev), -1e30, jnp.float32)
        shard_cols = lax.all_gather(forward_value, "cap", axis=2, tiled=True)
        best = jnp.maximum(
            empty,
            best_reply(
                shard_cols.reshape(sec_dev * prod_count, shard_cols.shape[2]), row_first, cap_dev
            ),
        ).reshape(sec_dev, prod_count, cap_dev)
        values = jnp.where(live, relative[:, None, None] * output + best, scrap)
    return (values, relative)


def running_max(arr, lane, backward):
    width = arr.shape[1]

    def shifted(part, step):
        if backward:
            return jnp.where(lane < width - step, pltpu.roll(part, width - step, 1), NEG)
        return jnp.where(lane >= step, pltpu.roll(part, step, 1), NEG)

    arr = shifted(arr, 1)
    step = 1
    while step < width:
        arr = jnp.maximum(arr, shifted(arr, step))
        step *= 2
    return arr


def undominated(gain, square, t_low, t_high, lane):
    low = gain - square * t_low
    high = gain - square * t_high
    return (low > running_max(low, lane, False)) & (high > running_max(high, lane, True))


def compress(keep, before, lane, gain, extra=None):
    width = gain.shape[1]
    shift = jnp.where(keep, lane - before, 0)
    gain = jnp.where(keep, gain, NEG)
    left = shift
    step = 1
    while step < width:
        move_gain = pltpu.roll(gain, width - step, 1)
        move_left = pltpu.roll(left, width - step, 1)
        arrive = (move_left & step) != 0
        leave = (left & step) != 0
        gain = jnp.where(arrive, move_gain, jnp.where(leave, NEG, gain))
        if extra is not None:
            extra = jnp.where(arrive, pltpu.roll(extra, width - step, 1), extra)
        left = jnp.where(arrive, move_left, jnp.where(leave, 0, left))
        step *= 2
    return gain, left if extra is None else extra


def sweeps_kernel(n_sec, n_cap, start_ref, mass_ref, survive_ref, exit_ref, demand_ref, trans_ref, cost_ref,
                  value_ref, rel_ref, flag_ref,
                  out_ref, forward_ref, tri_ref, wide_ref, over_ref, part_ref, parts_ref, pay_ref, pays_ref,
                  root_ref, roots_ref, mark_ref, marks_ref, best_ref, mark_send, mark_recv, part_send, part_recv, pay_send, pay_recv, root_send, root_recv):
    sec_dev, prods, cap_dev = start_ref.shape
    total = cap_dev * n_cap
    me_cap = lax.axis_index("cap")
    me_sec = lax.axis_index("sector")
    mesh_id = pl.DeviceIdType.MESH

    barrier = pltpu.get_barrier_semaphore()
    for off in range(1, n_cap):
        pl.semaphore_signal(barrier, inc=1, device_id={"cap": lax.rem(me_cap + off, n_cap)}, device_id_type=mesh_id)
    for off in range(1, n_sec):
        pl.semaphore_signal(barrier, inc=1, device_id={"sector": lax.rem(me_sec + off, n_sec)}, device_id_type=mesh_id)

    lane = lax.broadcasted_iota(jnp.int32, (prods, cap_dev), 1)
    lane_one = lax.broadcasted_iota(jnp.int32, (1, cap_dev), 1)
    lane_tile = lax.broadcasted_iota(jnp.int32, (prods, 128), 1)
    prod_col = lax.broadcasted_iota(jnp.int32, (prods, cap_dev), 0)
    first = me_cap * cap_dev
    capital = capital_of(first + lane_one, total)
    slope = 1.0 / capital
    scrap = 0.3 * capital
    power = jnp.exp(0.6 * (math.log(0.2) + math.log(10.0) * (first + lane_one).astype(jnp.float32) / (total - 1)))
    out_ref[...] = jnp.exp(-0.5 + prod_col.astype(jnp.float32) / (prods - 1)) * power
    tri_ref[...] = (
        lax.broadcasted_iota(jnp.int32, tri_ref.shape, 0) < lax.broadcasted_iota(jnp.int32, tri_ref.shape, 1)
    ).astype(jnp.bfloat16)
    t_low, t_high = 1.0 / 2.0, 1.0 / 0.2
    halves = sec_dev // 4
    merged_width = 128 * pl.cdiv(n_cap, 4)
    lane_merged = lax.broadcasted_iota(jnp.int32, (prods, merged_width), 1)
    own_low = jnp.broadcast_to(slope[:, cap_dev - 1:cap_dev], (prods, merged_width))
    own_high = jnp.broadcast_to(slope[:, 0:1], (prods, merged_width))
    over_ref[...] = jnp.zeros_like(over_ref)

    def live_of(s):
        return (survive_ref[s] == 1) & (prod_col >= exit_ref[s])

    copies = []
    pl.semaphore_wait(barrier, n_cap - 1 + n_sec - 1)
    for sweep in range(SWEEPS):
        source = start_ref if sweep == 0 else value_ref

        def supply_step(s, carry):
            stay = jax.nn.sigmoid((source[s] - scrap) / 0.5)
            weighted = jnp.where(live_of(s), mass_ref[s] * stay * out_ref[...], 0.0)
            row = jnp.sum(weighted, axis=0, keepdims=True)
            folded = row[:, 0:128]
            for at in range(128, cap_dev, 128):
                folded = folded + row[:, at:at + 128]
            part_ref[sweep, pl.ds(s, 1), :] = folded
            return carry

        lax.fori_loop(0, sec_dev, supply_step, 0)
        part_copies = []
        for off in range(1, n_cap):
            part_copies.append(pltpu.make_async_remote_copy(
                src_ref=part_ref.at[sweep], dst_ref=parts_ref.at[sweep, me_cap],
                send_sem=part_send.at[sweep, off - 1], recv_sem=part_recv.at[sweep, off - 1],
                device_id={"cap": lax.rem(me_cap + off, n_cap)}, device_id_type=mesh_id))
            part_copies[-1].start()
        parts_ref[sweep, me_cap] = part_ref[sweep]

        pay_ref[sweep] = jnp.full(pay_ref.shape[1:], NEG, jnp.float32)

        def forward_step(s, carry):
            vals = source[s]
            cont = jnp.where(live_of(s), jnp.maximum(vals, scrap), scrap)
            expect = jnp.dot(trans_ref[...], cont, precision=lax.Precision.HIGHEST, preferred_element_type=jnp.float32)
            forward = 0.9 * expect - cost_ref[...]
            forward_ref[s] = forward
            gain = forward + 0.8 * capital
            keep = undominated(gain, capital * capital, t_low, t_high, lane)
            before = jnp.dot(keep.astype(jnp.bfloat16), tri_ref[0:cap_dev, 0:cap_dev], preferred_element_type=jnp.float32)
            packed, moved = compress(keep, before.astype(jnp.int32), lane, gain)
            packed, moved = packed[:, 0:128], moved[:, 0:128]
            over_ref[...] = jnp.maximum(over_ref[...], jnp.where((lane_tile == SLOTS) & (packed > 0.5 * NEG), 1.0, 0.0))
            square = capital_of(first + lane_tile + moved, total)
            square = jnp.where(packed > 0.5 * NEG, square * square, 0.0)
            both = jnp.where(lane_tile < SLOTS, packed, pltpu.roll(square, SLOTS, 1))
            group = s // halves
            rows = pl.ds(pl.multiple_of((s % halves) * prods, prods), prods)
            placed = pltpu.roll(both, group * (2 * SLOTS), 1)
            pay_ref[sweep, rows, :] = jnp.where(lane_tile // (2 * SLOTS) == group, placed, pay_ref[sweep, rows, :])
            return carry

        def flags_so_far():
            flags = over_ref[0:8, :]
            for at in range(8, prods, 8):
                flags = jnp.maximum(flags, over_ref[at:at + 8, :])
            return flags

        lax.fori_loop(0, sec_dev, forward_step, 0)
        flags = flags_so_far()
        pay_ref[sweep, halves * prods:halves * prods + 8, :] = flags
        pay_copies = []
        for off in range(1, n_cap):
            pay_copies.append(pltpu.make_async_remote_copy(
                src_ref=pay_ref.at[sweep], dst_ref=pays_ref.at[sweep, me_cap],
                send_sem=pay_send.at[sweep, off - 1], recv_sem=pay_recv.at[sweep, off - 1],
                device_id={"cap": lax.rem(me_cap + off, n_cap)}, device_id_type=mesh_id))
            pay_copies[-1].start()
        pays_ref[sweep, me_cap] = pay_ref[sweep]

        for copy in part_copies:
            copy.wait_recv()
        gathered = parts_ref[sweep, 0]
        for d in range(1, n_cap):
            gathered = gathered + parts_ref[sweep, d]
        supply = 1.0 + jnp.sum(gathered, axis=1, keepdims=True) / (prods * total)
        prices = jnp.sqrt(demand_ref[...] / supply)
        for copy in pay_copies:
            copy.wait_recv()
        flag_rows = pl.ds(halves * prods, 8)
        flags = pays_ref[sweep, 0, flag_rows, :]
        for d in range(1, n_cap):
            flags = jnp.maximum(flags, pays_ref[sweep, d, flag_rows, :])

        def select_step(part, carry):
            merged = []
            for k in range(sec_dev // 2):
                s = part * (sec_dev // 2) + k
                group = s // halves
                rows = pl.ds(pl.multiple_of((s % halves) * prods, prods), prods)
                tiles = []
                for d in range(n_cap):
                    turn = lax.rem((d % 4) * (2 * SLOTS) + 128 - group * (2 * SLOTS), 128)
                    block = pltpu.roll(pays_ref[sweep, d, rows, :], turn, 1)
                    if d % 4 == 0:
                        tiles.append(jnp.where(lane_tile < 2 * SLOTS, block, NEG))
                    else:
                        tiles[-1] = jnp.where(lane_tile // (2 * SLOTS) == d % 4, block, tiles[-1])
                merged.append(tiles[0] if len(tiles) == 1 else jnp.concatenate(tiles, axis=1))
            merged = jnp.concatenate(merged, axis=0)
            lanes = lax.broadcasted_iota(jnp.int32, merged.shape, 1)
            gain = jnp.where(lanes % (2 * SLOTS) < SLOTS, merged, NEG)
            square = jnp.where(gain > 0.5 * NEG, pltpu.roll(merged, merged_width - SLOTS, 1), 0.0)
            keep = undominated(gain, square, own_low[0:1], own_high[0:1], lanes) & (gain > 0.5 * NEG)
            before = jnp.dot(keep.astype(jnp.bfloat16), tri_ref[0:merged_width, 0:merged_width], preferred_element_type=jnp.float32)
            packed, square = compress(keep, before.astype(jnp.int32), lanes, gain, square)
            packed, square = packed[:, 0:128], square[:, 0:128]
            both = jnp.where(lanes[:, 0:128] < OWN_SLOTS, packed, pltpu.roll(square, OWN_SLOTS, 1))
            for k in range(sec_dev // 2):
                cut = packed[k * prods:(k + 1) * prods]
                over_ref[...] = jnp.maximum(over_ref[...], jnp.where((lane_tile == OWN_SLOTS) & (cut > 0.5 * NEG), 1.0, 0.0))
                best_ref[part * (sec_dev // 2) + k] = both[k * prods:(k + 1) * prods]
            return carry

        def best_step(s, carry):
            block = best_ref[s]
            best = jnp.full((prods, cap_dev), NEG, jnp.float32)
            for c in range(OWN_SLOTS):
                best = jnp.maximum(best, block[:, c:c + 1] - block[:, OWN_SLOTS + c:OWN_SLOTS + c + 1] * slope)
            forward_ref[s] = jnp.maximum(best - 1.41 * capital, forward_ref[s] - 0.11 * capital)
            return carry

        mark_copies = []
        if sweep == SWEEPS - 1:
            lax.fori_loop(0, 2, select_step, 0)
            mark_ref[...] = jnp.maximum(flags, flags_so_far())
            for off in range(1, n_cap):
                mark_copies.append(pltpu.make_async_remote_copy(
                    src_ref=mark_ref, dst_ref=marks_ref.at[me_cap],
                    send_sem=mark_send.at[off - 1], recv_sem=mark_recv.at[off - 1],
                    device_id={"cap": lax.rem(me_cap + off, n_cap)}, device_id_type=mesh_id))
                mark_copies[-1].start()
            marks_ref[me_cap] = mark_ref[...]
            lax.fori_loop(0, sec_dev, best_step, 0)
            for copy in mark_copies:
                copy.wait_recv()
            for d in range(n_cap):
                flags = jnp.maximum(flags, marks_ref[d])

        root_ref[sweep, 0:sec_dev, :] = jnp.broadcast_to(jnp.sqrt(prices), (sec_dev, 128))
        root_ref[sweep, sec_dev:sec_dev + 8, :] = flags
        root_copies = []
        for off in range(1, n_sec):
            root_copies.append(pltpu.make_async_remote_copy(
                src_ref=root_ref.at[sweep], dst_ref=roots_ref.at[sweep, me_sec],
                send_sem=root_send.at[sweep, off - 1], recv_sem=root_recv.at[sweep, off - 1],
                device_id={"sector": lax.rem(me_sec + off, n_sec)}, device_id_type=mesh_id))
            root_copies[-1].start()
        roots_ref[sweep, me_sec] = root_ref[sweep]

        if sweep < SWEEPS - 1:
            lax.fori_loop(0, 2, select_step, 0)
            lax.fori_loop(0, sec_dev, best_step, 0)

        for copy in root_copies:
            copy.wait_recv()
        root_sum = roots_ref[sweep, 0]
        for d in range(1, n_sec):
            root_sum = root_sum + roots_ref[sweep, d]
        mean = jnp.sum(root_sum[0:sec_dev], axis=0, keepdims=True) / (sec_dev * n_sec)
        relative = prices / (mean[:, 0:1] * mean[:, 0:1])
        wide_ref[...] = jnp.broadcast_to(relative, (sec_dev, cap_dev))

        def value_step(s, carry):
            value_ref[s] = jnp.where(live_of(s), wide_ref[pl.ds(s, 1), :] * out_ref[...] + forward_ref[s], scrap)
            return carry

        lax.fori_loop(0, sec_dev, value_step, 0)
        copies += part_copies + pay_copies + root_copies + mark_copies
    rel_ref[...] = jnp.broadcast_to(relative, (sec_dev, 128))
    flag_ref[...] = root_sum[sec_dev:sec_dev + 8]
    for copy in copies:
        copy.wait_send()


def pruned_sweeps(start_value, firm_mass, survive, exit_index, demand, transition, install_cost):
    n_sec, n_cap = lax.axis_size("sector"), lax.axis_size("cap")
    sec_dev, prods, cap_dev = start_value.shape
    pay_rows = sec_dev // 4 * prods + 8
    merged_width = 128 * pl.cdiv(n_cap, 4)
    vmem = pl.BlockSpec(memory_space=pltpu.VMEM)
    smem = pl.BlockSpec(memory_space=pltpu.SMEM)
    f32 = jnp.float32
    return pl.pallas_call(
        functools.partial(sweeps_kernel, n_sec, n_cap),
        out_shape=(
            jax.ShapeDtypeStruct(start_value.shape, f32),
            jax.ShapeDtypeStruct((sec_dev, 128), f32),
            jax.ShapeDtypeStruct((8, 128), f32),
        ),
        in_specs=[vmem, vmem, vmem, smem, vmem, vmem, vmem],
        out_specs=(vmem, vmem, vmem),
        scratch_shapes=[
            pltpu.VMEM((prods, cap_dev), f32),
            pltpu.VMEM(start_value.shape, f32),
            pltpu.VMEM((max(cap_dev, merged_width),) * 2, jnp.bfloat16),
            pltpu.VMEM((sec_dev, cap_dev), f32),
            pltpu.VMEM((prods, 128), f32),
            pltpu.VMEM((SWEEPS, sec_dev, 128), f32),
            pltpu.VMEM((SWEEPS, n_cap, sec_dev, 128), f32),
            pltpu.VMEM((SWEEPS, pay_rows, 128), f32),
            pltpu.VMEM((SWEEPS, n_cap, pay_rows, 128), f32),
            pltpu.VMEM((SWEEPS, sec_dev + 8, 128), f32),
            pltpu.VMEM((SWEEPS, n_sec, sec_dev + 8, 128), f32),
            pltpu.VMEM((8, 128), f32),
            pltpu.VMEM((n_cap, 8, 128), f32),
            pltpu.VMEM((sec_dev, prods, 128), f32),
            pltpu.SemaphoreType.DMA((n_cap - 1,)),
            pltpu.SemaphoreType.DMA((n_cap - 1,)),
            pltpu.SemaphoreType.DMA((SWEEPS, n_cap - 1)),
            pltpu.SemaphoreType.DMA((SWEEPS, n_cap - 1)),
            pltpu.SemaphoreType.DMA((SWEEPS, n_cap - 1)),
            pltpu.SemaphoreType.DMA((SWEEPS, n_cap - 1)),
            pltpu.SemaphoreType.DMA((SWEEPS, n_sec - 1)),
            pltpu.SemaphoreType.DMA((SWEEPS, n_sec - 1)),
        ],
        compiler_params=pltpu.CompilerParams(
            collective_id=0, has_side_effects=True, vmem_limit_bytes=48 * 1024 * 1024
        ),
    )(start_value, firm_mass, survive, exit_index, demand[:, None], transition, install_cost[None, :])


def on_device(start_value, firm_mass, survive, exit_index, demand, transition, install_cost):
    args = (start_value, firm_mass, survive, exit_index, demand, transition, install_cost)
    sec_dev, prods, cap_dev = start_value.shape
    if sec_dev % 8 or prods % 8 or cap_dev % 128 or min(lax.axis_size("sector"), lax.axis_size("cap")) < 2:
        return dense_sweeps(*args)
    values, relative, flags = pruned_sweeps(*args)
    return lax.cond(
        jnp.max(flags) > 0.0,
        lambda: dense_sweeps(*args),
        lambda: (values, relative[:, 0]),
    )


def solution(mesh):
    return jax.shard_map(
        on_device,
        mesh=mesh,
        in_specs=(
            P("sector", None, "cap"),
            P("sector", None, "cap"),
            P("sector", None, "cap"),
            P("sector"),
            P("sector"),
            P(),
            P("cap"),
        ),
        out_specs=(P("sector", None, "cap"), P("sector")),
        check_vma=False,
    )
```
